32 devices in a mesh: layer: 8 (over z, x), plane: 4 (over y, core).
Axes of the slice: x: 2, y: 2, z: 4, core: 2. Of those that a mesh axis runs over, the one named last changes fastest.
Arguments:
- sources: float32 [8, 16, 4096], P('layer', None, 'plane'), may hold values from -6 to 6
- fronts: float32 [8, 32, 128, 128], P('layer', 'plane'), as said below
- down_left: bfloat16 [8, 4, 128, 4096], P('layer', None, None, 'plane'), may hold values from -0.1875 to 0.1875
- down_right: bfloat16 [8, 4, 128, 4096], P('layer', None, None, 'plane'), may hold values from -0.4375 to 0.4375
- up_left: bfloat16 [8, 4, 128, 4096], P('layer', None, None, 'plane'), may hold values from -0.1875 to 0.1875
- up_right: bfloat16 [8, 4, 128, 4096], P('layer', None, None, 'plane'), may hold values from -0.4375 to 0.4375
- ranks: int32 [8, 2, 4, 4], P('layer', None, 'plane'), may hold values from 1 to 128
- pattern: int32 [8, 2, 4, 4], P('layer', None, 'plane'), may hold values 0 or 1
Outputs:
- field: float32 [8, 16, 4096], P('layer', None, 'plane')
The draws below stay inside these ranges and needn't reach their ends.
Inputs may be any that keep to these rules, and one draw needn't show every extreme that they name: fronts[l, b] is lower triangular with every diagonal entry between 1 and 4.
All inputs are finite; a program needn't handle non-finite values. No bound on the sum of `pattern` on one device may be relied on, other than what follows from the above.
Results may differ from the reference program's by a relative error of at most 0.025.
Values may be sent and summed in bfloat16 or wider, within the bound.
No kernel may reach another device: no remote copies, remote signals or barrier semaphores. Data moves between devices by JAX's collectives and lax.ppermute only.
A program may use at most 64 MiB of HBM per device.

```python
import math
import jax
import jax.numpy as jnp
from jax import lax

TILE = 1024
SOURCES = 16
RMAX = 128
BLK = 128
NT = 4
W = 4096
LAYERS = 8


def draw_fronts(key, part):
    first_key, second_key = jax.random.split(jax.random.fold_in(key, 17))
    shape = (LAYERS, W // BLK, BLK, BLK)
    lower = jax.random.normal(first_key, shape, jnp.float32) * (0.3 / math.sqrt(BLK))
    diagonal = jax.random.uniform(second_key, shape[:3], jnp.float32, 1.0, 2.0)
    identity = jnp.eye(BLK, dtype=jnp.float32)
    return jnp.tril(lower, -1) + diagonal[..., None] * identity


def set_ends(values, own_key, least, top_value):
    shape = values.shape
    index_at = [jax.random.randint(jax.random.fold_in(own_key, axis), (), 0, shape[axis]) for axis in range(len(shape))]
    values = values.at[tuple(index_at)].set(least)
    longest = shape.index(max(shape))
    index_at[longest] = (index_at[longest] + 1) % shape[longest]
    return values.at[tuple(index_at)].set(top_value)


def block_levels(own_key, shape, shards, least, top_value):
    level = 1.0
    for position, shards_of in shards:
        heights = jax.random.uniform(jax.random.fold_in(jax.random.fold_in(own_key, 6), position), (shards_of,), jnp.float32, least / len(shards), top_value / len(shards))
        level = level * jnp.repeat(jnp.exp(heights), shape[position] // shards_of).reshape((-1,) + (1,) * (len(shape) - 1 - position))
    return level


def bell_draw(rng, extent, deviation, reach, pieces=(), kind=jnp.bfloat16):
    level = block_levels(rng, extent, pieces, -0.22, 0.18) if pieces else 1.0
    drawn = jax.random.normal(rng, extent, jnp.float32) * deviation * level
    return jnp.minimum(jnp.maximum(drawn, -reach), reach).astype(kind)


def setup_inputs(seed: int = 0) -> dict:
    keys = jax.random.split(jax.random.key(seed), 9)
    return {
        "sources": bell_draw(keys[0], (LAYERS, SOURCES, W), 1.0, 6.0, ((0, 8), (2, 4)), jnp.float32),
        "fronts": draw_fronts(jax.random.fold_in(keys[8], 71), 0),
        "down_left": bell_draw(keys[2], (LAYERS, NT, RMAX, W), TILE ** -0.5, 0.1875, ((0, 8), (3, 4))),
        "down_right": bell_draw(keys[3], (LAYERS, NT, RMAX, W), (NT * RMAX * 3 // 7) ** -0.5, 0.4375, ((0, 8), (3, 4))),
        "up_left": bell_draw(keys[4], (LAYERS, NT, RMAX, W), TILE ** -0.5, 0.1875, ((0, 8), (3, 4))),
        "up_right": bell_draw(keys[5], (LAYERS, NT, RMAX, W), (NT * RMAX * 3 // 7) ** -0.5, 0.4375, ((0, 8), (3, 4))),
        "ranks": set_ends(jax.random.randint(keys[6], (LAYERS, 2, NT, NT), 1, RMAX + 1), jax.random.fold_in(keys[6], 1), 1, RMAX).astype(jnp.int32),
        "pattern": set_ends((jax.random.randint(keys[7], (LAYERS, 2, NT, NT), 0, 4) < 3).astype(jnp.int32), jax.random.fold_in(keys[7], 1), 0, 1),
    }


def front_solve(source, front_blocks):
    stacked = source.reshape(source.shape[0], front_blocks.shape[0], front_blocks.shape[1]).transpose(1, 2, 0)
    solved = jax.scipy.linalg.solve_triangular(front_blocks, stacked, lower=True)
    return solved.transpose(2, 0, 1).reshape(source.shape)

def transfer(trace, factor_in, factor_out, rank_rows, present):
    rounded = trace.astype(jnp.bfloat16).astype(jnp.float32).reshape(SOURCES, NT, TILE)
    left_full = factor_in.astype(jnp.float32).reshape(NT, RMAX, NT, TILE)
    coeffs = jnp.einsum('ikjt,sjt->ijsk', left_full, rounded, precision=lax.Precision.HIGHEST)
    coeffs = coeffs.astype(jnp.bfloat16).astype(jnp.float32)
    ladder = jnp.arange(RMAX, dtype=jnp.int32)
    keep_mask = present[:, :, None].astype(jnp.float32) * (ladder[None, None, :] < rank_rows[:, :, None]).astype(jnp.float32)
    coeffs = coeffs * keep_mask[:, :, None, :]
    right_full = factor_out.astype(jnp.float32).reshape(NT, RMAX, NT, TILE)
    result = jnp.einsum('ijsk,jkit->sit', coeffs, right_full, precision=lax.Precision.HIGHEST)
    return result.reshape(SOURCES, W)

def reference(sources, fronts, down_left, down_right, up_left, up_right, ranks, pattern):
    solved = jax.vmap(front_solve)(sources, fronts)

    def sweep_step(previous, items):
        local_part, factor_in, factor_out, rank_rows, present = items
        nxt = local_part + transfer(previous, factor_in, factor_out, rank_rows, present)
        return (nxt, nxt)
    start = jnp.zeros((SOURCES, W), jnp.float32)
    _, down = lax.scan(sweep_step, start, (solved, down_left, down_right, ranks[:, 0], pattern[:, 0]))
    _, upward = lax.scan(sweep_step, start, (solved, up_left, up_right, ranks[:, 1], pattern[:, 1]), reverse=True)
    return down + upward - solved
```

```python
import functools

import jax
import jax.numpy as jnp
from jax import lax
from jax.experimental import pallas as pl
from jax.experimental.pallas import tpu as pltpu
from jax.sharding import PartitionSpec as P


def solve_kernel(source_ref, front_ref, out_ref):
    blocks, size, _ = front_ref.shape
    row = lax.broadcasted_iota(jnp.int32, (size, size), 0)
    col = lax.broadcasted_iota(jnp.int32, (size, size), 1)
    state, lower = [], []
    for b in range(blocks):
        turned = front_ref[b].T
        diagonal = jnp.sum(jnp.where(row == col, turned, 0.0), axis=0, keepdims=True)
        scale = 1.0 / diagonal
        lower.append(jnp.where(row < col, turned * scale, 0.0))
        state.append(source_ref[:, b * size : (b + 1) * size] * scale)
    for t in range(size - 1):
        for b in range(blocks):
            state[b] = state[b] - state[b][:, t : t + 1] * lower[b][t : t + 1, :]
    for b in range(blocks):
        out_ref[:, b * size : (b + 1) * size] = state[b]


def front_solve(source, front_blocks):
    return pl.pallas_call(
        solve_kernel,
        out_shape=jax.ShapeDtypeStruct(source.shape, jnp.float32),
        in_specs=[pl.BlockSpec(memory_space=pltpu.VMEM)] * 2,
        out_specs=pl.BlockSpec(memory_space=pltpu.VMEM),
        compiler_params=pltpu.CompilerParams(vmem_limit_bytes=16 * 2**20),
        name="front_solve",
    )(source, front_blocks)


def compress(trace, factor_in):
    return jnp.einsum(
        "ikt,st->isk", factor_in, trace, preferred_element_type=jnp.float32
    ).astype(jnp.bfloat16)


def expand(coeffs, factor_out, keep_mask):
    return jnp.einsum(
        "jsk,jkt->st",
        coeffs * keep_mask[:, None, :],
        factor_out,
        preferred_element_type=jnp.float32,
    )


def shards(layers, planes, sources, fronts, down_left, down_right, up_left, up_right, ranks, pattern):
    solved = front_solve(sources[0], fronts[0])
    layer_at = lax.axis_index("layer")
    rank_top = down_left.shape[2]
    ladder = jnp.arange(rank_top, dtype=jnp.int32)
    keep_mask = (
        pattern[0, :, 0, :, None]
        * (ladder[None, None, :] < ranks[0, :, 0, :, None]).astype(jnp.int32)
    ).astype(jnp.bfloat16)

    half = layers // 2
    down_first = layer_at < half
    lefts = (
        jnp.where(down_first, down_left[0], up_left[0]),
        jnp.where(down_first, up_left[0], down_left[0]),
    )
    rights = (
        jnp.where(down_first, down_right[0], up_right[0]),
        jnp.where(down_first, up_right[0], down_right[0]),
    )
    keeps = (
        jnp.where(down_first, keep_mask[0], keep_mask[1]),
        jnp.where(down_first, keep_mask[1], keep_mask[0]),
    )

    trace = solved
    results = [solved, solved]
    for turn in range(layers - 1):
        which = 0 if turn < half - 1 else 1
        pairs = []
        for plane in range(planes):
            pairs.append((turn * planes + plane, (turn + 1) * planes + plane))
            pairs.append(((layers - 1 - turn) * planes + plane, (layers - 2 - turn) * planes + plane))
        arrived = lax.ppermute(trace.astype(jnp.bfloat16), ("layer", "plane"), pairs)
        coeffs = compress(arrived, lefts[which])
        coeffs = lax.all_to_all(coeffs, "plane", split_axis=0, concat_axis=0, tiled=True)
        trace = solved + expand(coeffs, rights[which], keeps[which])
        active = (layer_at == turn + 1) | (layer_at == layers - 2 - turn)
        results[which] = jnp.where(active, trace, results[which])
    field = results[0] + results[1] - solved
    return field[None]


def solution(mesh):
    layers, planes = mesh.shape["layer"], mesh.shape["plane"]
    in_specs = (
        P("layer", None, "plane"),
        P("layer", "plane", None, None),
        P("layer", None, None, "plane"),
        P("layer", None, None, "plane"),
        P("layer", None, None, "plane"),
        P("layer", None, None, "plane"),
        P("layer", None, "plane", None),
        P("layer", None, "plane", None),
    )
    out_specs = P("layer", None, "plane")
    return jax.shard_map(
        functools.partial(shards, layers, planes),
        mesh=mesh,
        in_specs=in_specs,
        out_specs=out_specs,
        check_vma=False,
    )
```
